32 devices in a mesh: rep: 1, dp: 32 (over x, y, z, core).
Axes of the slice: x: 2, y: 2, z: 4, core: 2. Of those that a mesh axis runs over, the one named last changes fastest.
Arguments:
- x: bfloat16 [32, 2048, 896], P(('rep', 'dp'))
- dy: bfloat16 [32, 2048, 896], P(('rep', 'dp'))
- w_gate: bfloat16 [2, 896, 2304], P(None, 'dp')
- w_up: bfloat16 [2, 896, 2304], P(None, 'dp')
- w_down: bfloat16 [2, 2304, 896], P(None, 'dp')
Outputs:
- output 1: bfloat16 [32, 2048, 896], P(('rep', 'dp'))
- output 2: bfloat16 [2, 896, 2304], P('rep', 'dp')
- output 3: bfloat16 [2, 896, 2304], P('rep', 'dp')
- output 4: bfloat16 [2, 2304, 896], P('rep', 'dp')
All inputs are finite; a program needn't handle non-finite values.
Results may differ from the reference program's by a relative error of at most 0.018.
Values are sent between devices in bfloat16 or wider.
A program may use at most 2 GiB of HBM per device.

```python
import jax
import jax.numpy as jnp
from jax import lax

SEQUENCES = 32
TOKENS = 2048
D = 896
FF = 2304
LAYERS = 2
NAMES = ("w_gate", "w_up", "w_down")
SHAPES = {"w_gate": (LAYERS, D, FF), "w_up": (LAYERS, D, FF), "w_down": (LAYERS, FF, D)}


def bump(key, n, height):
    away = (jnp.arange(n, dtype=jnp.int32) - jax.random.randint(key, (), 0, n, jnp.int32)) % n
    return jnp.where(away < n // 8, height, 1.0)


def together(key, own, strength):
    shared = jax.random.normal(key, own.shape[1:], jnp.float32)
    return (own + strength * shared) * lax.rsqrt(1 + strength * strength)


def setup_inputs(seed: int = 0, part: int = 0) -> dict:
    kx, kdy, ka, kb, kz, kf, kh, kl, *kw = jax.random.split(jax.random.key(seed), 8 + len(NAMES))
    kx, kdy, ka, kb = (jax.random.fold_in(k, part) for k in (kx, kdy, ka, kb))
    shape = (SEQUENCES, TOKENS, D)
    much_x, much_dy = jax.random.uniform(kz, (2,), jnp.float32, 0.0, 1.0)
    layers = 2.0 ** jax.random.uniform(kl, (LAYERS, 1, 1), jnp.float32, -1.0, 1.0)
    x = together(ka, jax.random.normal(kx, shape, jnp.float32), much_x) * bump(kf, D, 4.0)
    dy = together(kb, jax.random.normal(kdy, shape, jnp.float32), much_dy)
    drawn = {"x": x.astype(jnp.bfloat16), "dy": (dy * (SEQUENCES * TOKENS) ** -0.5).astype(jnp.bfloat16)}
    for key, name in zip(kw, NAMES, strict=True):
        w = jax.random.normal(key, SHAPES[name], jnp.float32) * SHAPES[name][1] ** -0.5
        drawn[name] = (w * {"w_gate": 1.0, "w_up": bump(kh, FF, 4.0), "w_down": layers}[name]).astype(jnp.bfloat16)
    return drawn


def matmul(a, w):
    return jnp.dot(a, w, preferred_element_type=jnp.float32).astype(jnp.bfloat16)


def normed(h):
    wide = h.astype(jnp.float32)
    scale = lax.rsqrt(jnp.mean(wide**2, -1, keepdims=True) + 1e-6)
    return (wide * scale).astype(jnp.bfloat16)


def layer(h, w):
    a = normed(h)
    gate = jnp.dot(a, w["w_gate"], preferred_element_type=jnp.float32)
    up = jnp.dot(a, w["w_up"], preferred_element_type=jnp.float32)
    return h + matmul((jax.nn.silu(gate) * up).astype(jnp.bfloat16), w["w_down"])


def stack(weights, h):
    return lax.scan(lambda h, w: (layer(h, w), None), h, weights)[0]


def reference(x, dy, w_gate, w_up, w_down):
    weights = dict(zip(NAMES, (w_gate, w_up, w_down), strict=True))

    def take(so_far, sequence):
        h, by_y = sequence
        _, back = jax.vjp(stack, weights, h)
        by_weights, by_h = back(by_y)
        return jax.tree.map(lambda total, term: total + term.astype(jnp.float32), so_far, by_weights), by_h

    none_yet = {name: jnp.zeros(w.shape, jnp.float32) for name, w in weights.items()}
    by_weights, by_x = lax.scan(take, none_yet, (x, dy))
    return (by_x, *(by_weights[name].astype(jnp.bfloat16) for name in NAMES))
```

```python
import jax
import jax.numpy as jnp
from jax import lax
from jax.sharding import PartitionSpec as P

EPS = 1e-6
F32, BF16 = jnp.float32, jnp.bfloat16


def dot(a, b, ca, cb):
    return lax.dot_general(a, b, (((ca,), (cb,)), ((), ())), preferred_element_type=F32)


def normed(h):
    wide = h.astype(F32)
    scale = lax.rsqrt(jnp.mean(wide**2, -1, keepdims=True) + EPS)
    return (wide * scale).astype(BF16)


def norm_back(h, by_a):
    wide, by_a = h.astype(F32), by_a.astype(F32)
    scale = lax.rsqrt(jnp.mean(wide**2, -1, keepdims=True) + EPS)
    return (scale * (by_a - wide * (scale * scale * jnp.mean(by_a * wide, -1, keepdims=True)))).astype(BF16)


def solution(mesh):
    devices = mesh.shape["dp"]

    def step(x, dy, w_gate, w_up, w_down):
        layers, rows, ff = w_gate.shape
        deep, d = w_down.shape[1:]
        size = rows * ff // 128
        parts = [t.reshape(layers, 1, size, 128) for t in (w_gate, w_up, w_down)]
        held = lax.all_gather(jnp.concatenate(parts, 1).reshape(layers * 3 * size, 128), "dp", axis=0)
        held = held.reshape(devices, layers, 3, size, 128)
        h, by_h = x[0], dy[0]
        kept = []
        for n in range(layers):
            wg, wu = (held[:, n, k].reshape(devices * rows, ff) for k in (0, 1))
            wd = held[:, n, 2].reshape(devices * deep, d)
            a = normed(h)
            gate, up = dot(a, wg, 1, 0), dot(a, wu, 1, 0)
            p = (jax.nn.silu(gate) * up).astype(BF16)
            kept.append((h, a, gate, up, p, wg, wu, wd))
            h = h + dot(p, wd, 1, 0).astype(BF16)
        by_weights = []
        for n in reversed(range(layers)):
            h, a, gate, up, p, wg, wu, wd = kept[n]
            by_p = dot(by_h, wd, 1, 1).astype(BF16).astype(F32)
            s = jax.nn.sigmoid(gate)
            by_up = (by_p * (gate * s)).astype(BF16)
            by_gate = (by_p * up * (s * (1 + gate * (1 - s)))).astype(BF16)
            terms = dot(a, by_gate, 0, 0), dot(a, by_up, 0, 0), dot(p, by_h, 0, 0)
            by_weights = [t.astype(BF16).reshape(devices, size, 128) for t in terms] + by_weights
            by_a = dot(by_gate, wg, 1, 1).astype(BF16) + dot(by_up, wu, 1, 1).astype(BF16)
            by_h = by_h + norm_back(h, by_a)
        sent = jnp.concatenate(by_weights, 1).reshape(-1, 128)
        own = lax.psum_scatter(sent, "dp", scatter_dimension=0, tiled=True).reshape(layers, 3, size, 128)
        return (by_h[None], *(own[:, k].reshape(w.shape) for k, w in enumerate((w_gate, w_up, w_down))))

    tokens, weights = P(("rep", "dp"), None, None), P(None, "dp", None)
    return jax.shard_map(
        step,
        mesh=mesh,
        in_specs=(tokens, tokens, weights, weights, weights),
        out_specs=(tokens, P("rep", "dp", None), P("rep", "dp", None), P("rep", "dp", None)),
        check_vma=False,
    )
```

```python
import functools

import jax
import jax.numpy as jnp
from jax import lax
from jax.experimental import pallas as pl
from jax.experimental.pallas import tpu as pltpu
from jax.sharding import PartitionSpec as P

EPS = 1e-6
F32, BF16 = jnp.float32, jnp.bfloat16
MESH = pl.DeviceIdType.MESH
ANY = pl.BlockSpec(memory_space=pl.ANY)
VMEM_LIMIT = 66_000_000


class Place:
    def __init__(self):
        me = lax.axis_index("dp")
        core, z = lax.rem(me, 2), lax.rem(me // 2, 4)
        column = me - 2 * z - core
        y, x = lax.rem(me // 8, 2), me // 16
        self.me, self.core, self.z = me, core, z
        self.partner = me + 1 - 2 * core
        self.by_x, self.by_y = me + 16 - 32 * x, me + 8 - 16 * y
        over_x, over_y = column + 16 - 32 * x, column + 8 - 16 * y
        self.columns = column, over_x, over_y, over_x + 8 - 16 * y
        self.in_z = [column + core + 2 * lax.rem(z + k, 4) for k in range(4)]

    def piece(self, kind, k, core=None):
        core = self.core if core is None else core
        return self.columns[kind] + 2 * lax.rem(self.z + 4 - k, 4) + core

    def greet(self):
        barrier = pltpu.get_barrier_semaphore()
        for other in (self.partner, self.by_x, self.by_y, *self.in_z[1:]):
            pl.semaphore_signal(barrier, inc=1, device_id={"dp": other}, device_id_type=MESH)
        pl.semaphore_wait(barrier, 6)


def remote(src, dst, send, recv, device):
    return pltpu.make_async_remote_copy(
        src_ref=src, dst_ref=dst, send_sem=send, recv_sem=recv, device_id={"dp": device}, device_id_type=MESH
    )


OWN, X, Y, DIAG = range(4)


class Gather:
    def __init__(self, place, src, out, send, recv, pair, local):
        self.place, self.src, self.out = place, src, out
        self.send, self.recv, self.pair, self.local = send, recv, pair, local

    def push(self, src, at, kind, k, device):
        remote(src, self.out.at[at], self.send, self.recv.at[4 * kind + k], device).start()

    def pass_on(self, src, at):
        remote(src, self.out.at[at], self.send, self.pair, self.place.partner).start()

    def start(self):
        place = self.place
        pltpu.make_async_copy(self.src, self.out.at[place.me], self.local).start()
        for k in (1, 2, 3):
            self.push(self.src, place.me, OWN, k, place.in_z[k])
        self.push(self.src, place.me, X, 0, place.by_x)
        self.push(self.src, place.me, Y, 0, place.by_y)
        self.pass_on(self.src, place.me)

    def arrived(self, kind, k):
        at = self.place.piece(kind, k)
        here = self.out.at[at]
        pltpu.make_async_copy(here, here, self.recv.at[4 * kind + k]).wait()
        return here, at

    def along_z(self, k):
        here, at = self.arrived(OWN, k)
        self.push(here, at, X, k, self.place.by_x)
        self.push(here, at, Y, k, self.place.by_y)
        self.pass_on(here, at)

    def across(self, k):
        here, at = self.arrived(X, k)
        if k < 2:
            self.push(here, at, DIAG, k, self.place.by_y)
        self.pass_on(here, at)
        here, at = self.arrived(Y, k)
        if k >= 2:
            self.push(here, at, DIAG, k, self.place.by_x)
        self.pass_on(here, at)

    def diagonal(self, k):
        self.pass_on(*self.arrived(DIAG, k))

    def finish(self):
        pltpu.make_async_copy(self.src, self.src, self.local).wait()
        for n, sem in ((16, self.pair), (31, self.send)):
            some = self.out.at[pl.ds(0, n)]
            pltpu.make_async_copy(some, some, sem).wait()

    def events(self):
        steps = [functools.partial(self.across, 0)]
        for k in (1, 2, 3):
            steps += [functools.partial(self.along_z, k), functools.partial(self.across, k)]
        return steps + [functools.partial(self.diagonal, k) for k in range(4)]


GATHER_SEMS = (pltpu.SemaphoreType.DMA, pltpu.SemaphoreType.DMA((16,)), pltpu.SemaphoreType.DMA, pltpu.SemaphoreType.DMA)


def woven(lists, lag):
    order = [(i + lag * n, n, step) for n, steps in enumerate(lists) for i, step in enumerate(steps)]
    return [step for _, _, step in sorted(order, key=lambda t: t[:2])]


class Scatter:
    def __init__(self, place, terms, out, mine, got, send, load, pair, cross, local):
        self.place, self.terms, self.out, self.mine, self.got = place, terms, out, mine, got
        self.send, self.load, self.pair, self.cross, self.local = send, load, pair, cross, local

    def start(self):
        place = self.place
        for kind in (DIAG, X, Y, OWN):
            for k in range(4):
                slot = 4 * kind + k
                src = self.terms.at[place.piece(kind, k, 1 - place.core)]
                remote(src, self.got.at[slot], self.send, self.pair.at[kind], place.partner).start()
                pltpu.make_async_copy(self.terms.at[place.piece(kind, k)], self.mine.at[slot], self.load.at[kind]).start()

    def ready(self, kind):
        four = self.mine.at[pl.ds(0, 4)]
        pltpu.make_async_copy(four, four, self.load.at[kind]).wait()
        pltpu.make_async_copy(four, four, self.pair.at[kind]).wait()

    def total(self, kind, k, others):
        slot = 4 * kind + k
        for n in others:
            here = self.got.at[16 + n]
            pltpu.make_async_copy(here, here, self.cross.at[n]).wait()
        total = self.mine[slot].astype(F32) + self.got[slot].astype(F32)
        for n in others:
            total += self.got[16 + n].astype(F32)
        return total.astype(BF16)

    def push(self, kind, k, others, to, device):
        slot = 4 * kind + k
        self.mine[slot] = self.total(kind, k, others)
        remote(self.mine.at[slot], self.got.at[16 + to], self.send, self.cross.at[to], device).start()

    def diagonal(self):
        self.ready(DIAG)
        for k in range(4):
            self.push(DIAG, k, (), k, self.place.by_x if k < 2 else self.place.by_y)

    def straight(self):
        self.ready(X)
        self.ready(Y)
        for k in (0, 1):
            self.push(X, k, (), 4 + k, self.place.by_x)
        for k in (2, 3):
            self.push(Y, k, (), 8 + k, self.place.by_y)

    def across(self):
        for k in (0, 1):
            self.push(Y, k, (k,), 8 + k, self.place.by_y)
        for k in (2, 3):
            self.push(X, k, (k,), 4 + k, self.place.by_x)

    def along_z(self):
        self.ready(OWN)
        for k in (1, 2, 3):
            self.push(OWN, k, (4 + k, 8 + k), 12 + k, self.place.in_z[4 - k])

    def last(self):
        self.mine[0] = self.total(OWN, 0, (4, 8, 13, 14, 15))
        pltpu.make_async_copy(self.mine.at[0], self.out, self.local).start()

    def events(self):
        return [self.diagonal, self.straight, self.across, self.along_z, self.last]

    def finish(self):
        pltpu.make_async_copy(self.mine.at[0], self.out, self.local).wait()
        some = self.terms.at[pl.ds(0, 31)]
        pltpu.make_async_copy(some, some, self.send).wait()


def scatter_scratch(terms):
    block = terms.shape[1:]
    dma = pltpu.SemaphoreType.DMA
    return [pltpu.VMEM((16, *block), BF16), pltpu.VMEM((32, *block), BF16), dma, dma((4,)), dma((4,)), dma((16,)), dma]


class Comm:
    def __init__(self, kind, arrays):
        self.kind, self.arrays, self.n = kind, list(arrays), len(arrays)
        if kind == "gather":
            self.shapes = [jax.ShapeDtypeStruct((32, *b.shape), BF16) for b in arrays]
            self.scratch = [s for _ in arrays for s in GATHER_SEMS]
        else:
            self.shapes = [jax.ShapeDtypeStruct(t.shape[1:], BF16) for t in arrays]
            self.scratch = [s for t in arrays for s in scatter_scratch(t)]
        self.specs = [ANY] * self.n

    def make(self, srcs, outs, scratch):
        place = Place()
        one = Gather if self.kind == "gather" else Scatter
        per = len(scratch) // max(self.n, 1)
        return place, [one(place, srcs[i], outs[i], *scratch[per * i : per * (i + 1)]) for i in range(self.n)]

    def drive(self, srcs, outs, scratch, step, steps):
        if not self.n:
            return
        place, ones = self.make(srcs, outs, scratch)
        events = woven([one.events() for one in ones], 3 if self.kind == "gather" else 1)

        @pl.when(step == 0)
        def _():
            place.greet()
            for one in ones:
                one.start()

        for i in range(steps):
            lo, hi = len(events) * i // steps, len(events) * (i + 1) // steps

            @pl.when(step == i)
            def _(lo=lo, hi=hi):
                for event in events[lo:hi]:
                    event()

        @pl.when(step == steps - 1)
        def _():
            for one in ones:
                one.finish()


NONE = Comm("gather", ())


def call(body, name, grid, ins, in_specs, outs, out_specs, scratch, comm, number, flops):
    n_in, n_out, n_scratch = len(ins), len(outs), len(scratch)

    def kernel(*refs):
        step = pl.program_id(0)
        cut = [n_in, comm.n, n_out, comm.n, n_scratch, len(comm.scratch)]
        groups, at = [], 0
        for c in cut:
            groups.append(refs[at : at + c])
            at += c
        srcs, sent = groups[1], groups[3]
        if body is not None:
            body(step, groups[0], groups[2], groups[4])
        comm.drive(srcs, sent, groups[5], step, grid)

    params = dict(vmem_limit_bytes=VMEM_LIMIT, dimension_semantics=("arbitrary",))
    if comm.n:
        params |= dict(collective_id=number, has_side_effects=True)
    results = pl.pallas_call(
        kernel,
        grid=(grid,),
        out_shape=[*outs, *comm.shapes],
        in_specs=[*in_specs, *comm.specs],
        out_specs=[*out_specs, *comm.specs],
        scratch_shapes=[*scratch, *comm.scratch],
        compiler_params=pltpu.CompilerParams(**params),
        cost_estimate=pl.CostEstimate(flops=flops, bytes_accessed=50_000_000, transcendentals=0),
        name=name,
    )(*ins, *comm.arrays)
    return list(results[:n_out]), list(results[n_out:])


def whole(shape):
    return pl.BlockSpec(shape, lambda i: (0,) * len(shape), pipeline_mode=pl.Buffered(1))


def over(rows, columns):
    return pl.BlockSpec((rows, columns), lambda i: (i, 0))


def across(rows, columns):
    return pl.BlockSpec((rows, columns), lambda i: (0, i))


def like(shape, dtype=BF16):
    return jax.ShapeDtypeStruct(shape, dtype)


def dot(a, b, ca, cb):
    return lax.dot_general(a, b, (((ca,), (cb,)), ((), ())), preferred_element_type=F32)


TILE = 256


def close_up(blocks, out):
    n, rows, _ = blocks.shape

    def pair(i, _):
        two = jnp.concatenate([blocks[2 * i].astype(F32), blocks[2 * i + 1].astype(F32)], 0)
        out[pl.ds(pl.multiple_of(2 * rows * i, 8), 2 * rows), :] = two.astype(BF16)
        return 0

    lax.fori_loop(0, n // 2, pair, 0)


def forward(h, wg, wu, wd, comm, number):
    tokens, d = h.shape
    n, rows, ff = wg.shape
    piece = ff // 3

    def body(step, ins, outs, scratch):
        h_ref, wg_ref, wu_ref, wd_ref = ins
        h_out, gate_ref, up_ref, pt_ref, at_ref, wg_out, wu_out = outs
        (p_ref,) = scratch

        @pl.when(step == 0)
        def _():
            close_up(wg_ref, wg_out)
            close_up(wu_ref, wu_out)

        wide = h_ref[...].astype(F32)
        a = (wide * lax.rsqrt(jnp.mean(wide**2, -1, keepdims=True) + EPS)).astype(BF16)
        at_ref[...] = a.T
        for c in range(3):
            part = pl.ds(piece * c, piece)
            gate = dot(a, wg_out[:, part], 1, 0)
            up = dot(a, wu_out[:, part], 1, 0)
            gate_ref[:, part] = gate
            up_ref[:, part] = up
            p = (gate * jax.nn.sigmoid(gate) * up).astype(BF16)
            p_ref[:, part] = p
            pt_ref[part, :] = p.T
        h_out[...] = h_ref[...] + dot(p_ref[...], wd_ref[...], 1, 0).astype(BF16)

    return call(
        body, f"forward_{number}", tokens // TILE,
        (h, wg, wu, wd),
        (over(TILE, d), whole(wg.shape), whole(wu.shape), whole(wd.shape)),
        (like(h.shape), like((tokens, ff), F32), like((tokens, ff), F32), like((ff, tokens)), like((d, tokens)),
         like((d, ff)), like((d, ff))),
        (over(TILE, d), over(TILE, ff), over(TILE, ff), across(ff, TILE), across(d, TILE), whole((d, ff)), whole((d, ff))),
        (pltpu.VMEM((TILE, ff), BF16),),
        comm, number, 6 * tokens * d * ff,
    )


def backward(by_h, h, gate, up, wg, wu, wd, comm, number):
    tokens, d = h.shape
    ff = gate.shape[1]
    piece = ff // 3

    def body(step, ins, outs, scratch):
        by_ref, h_ref, gate_ref, up_ref, wg_ref, wu_ref, wd_ref = ins
        by_gate_ref, by_up_ref, by_h_out = outs
        by_h = by_ref[...]
        for c in range(3):
            part = pl.ds(piece * c, piece)
            by_p = dot(by_h, wd_ref[part, :], 1, 1).astype(BF16).astype(F32)
            gate, up = gate_ref[:, part], up_ref[:, part]
            s = jax.nn.sigmoid(gate)
            by_up_ref[:, part] = (by_p * (gate * s)).astype(BF16)
            by_gate_ref[:, part] = (by_p * up * (s * (1 + gate * (1 - s)))).astype(BF16)
        by_a = dot(by_gate_ref[...], wg_ref[...], 1, 1).astype(BF16) + dot(by_up_ref[...], wu_ref[...], 1, 1).astype(BF16)
        wide, by_a = h_ref[...].astype(F32), by_a.astype(F32)
        scale = lax.rsqrt(jnp.mean(wide**2, -1, keepdims=True) + EPS)
        inner = jnp.mean(by_a * wide, -1, keepdims=True)
        by_h_out[...] = by_h + (scale * (by_a - wide * (scale * scale * inner))).astype(BF16)

    tile_d, tile_ff = over(TILE, d), over(TILE, ff)
    return call(
        body, f"backward_{number}", tokens // TILE,
        (by_h, h, gate, up, wg, wu, wd),
        (tile_d, tile_d, tile_ff, tile_ff, whole(wg.shape), whole(wu.shape), whole(wd.shape)),
        (like((tokens, ff)), like((tokens, ff)), like(h.shape)),
        (tile_ff, tile_ff, tile_d),
        (), comm, number, 6 * tokens * d * ff,
    )


def weight_terms(at, pt, by_gate, by_up, by_h, rows, comm, number):
    d, tokens = at.shape
    ff = pt.shape[0]
    n = d // rows

    def body(step, ins, outs, scratch):
        at_ref, pt_ref, by_gate_ref, by_up_ref, by_h_ref = ins
        wg_ref, wu_ref, wd_ref = outs
        for by_ref, w_ref in ((by_gate_ref, wg_ref), (by_up_ref, wu_ref)):
            term = dot(at_ref[...], by_ref[...], 1, 0)
            for j in range(n):
                w_ref[j] = term[rows * j : rows * j + rows].astype(BF16)
        wd_ref[...] = dot(pt_ref[...], by_h_ref[...], 1, 0).astype(BF16)

    blocks = pl.BlockSpec((n, rows, TILE), lambda i: (0, 0, i))
    return call(
        body, f"weight_terms_{number}", ff // TILE,
        (at, pt, by_gate, by_up, by_h),
        (whole(at.shape), over(TILE, tokens), across(tokens, TILE), across(tokens, TILE), whole(by_h.shape)),
        (like((n, rows, ff)), like((n, rows, ff)), like((ff, d))),
        (blocks, blocks, over(TILE, d)),
        (), comm, number, 6 * tokens * d * ff,
    )


def solution(mesh):
    def step(x, dy, w_gate, w_up, w_down):
        layers, rows, ff = w_gate.shape
        d = w_down.shape[2]
        own = [Comm("gather", (w_gate[n], w_up[n], w_down[n])) for n in range(layers)]
        _, held = call(None, "gather", 1, (), (), (), (), (), own[0], 0, 0)
        h, by_h = x[0], dy[0]
        kept = []
        for n in range(layers):
            wd = held[2].reshape(ff, d)
            (after, gate, up, pt, at, wg, wu), coming = forward(h, held[0], held[1], wd, own[n + 1] if n + 1 < layers else NONE, 1 + n)
            kept.append((h, gate, up, pt, at, wg, wu, wd))
            h, held = after, coming
        by_weights, terms = [], None
        for n in reversed(range(layers)):
            h, gate, up, pt, at, wg, wu, wd = kept[n]
            comm = NONE if terms is None else Comm("scatter", terms)
            (by_gate, by_up, before), summed = backward(by_h, h, gate, up, wg, wu, wd, comm, 8 + n)
            if terms is not None:
                by_weights.insert(0, summed)
            terms, _ = weight_terms(at, pt, by_gate, by_up, by_h, rows, NONE, 16 + n)
            terms[2] = terms[2].reshape(-1, *w_down.shape[1:])
            by_h = before
        _, summed = call(None, "scatter", 1, (), (), (), (), (), Comm("scatter", terms), 24, 0)
        by_weights.insert(0, summed)
        return (by_h[None], *(jnp.stack(t) for t in zip(*by_weights)))

    tokens, weights = P(("rep", "dp"), None, None), P(None, "dp", None)
    sums = P("rep", "dp", None)
    return jax.shard_map(
        step,
        mesh=mesh,
        in_specs=(tokens, tokens, weights, weights, weights),
        out_specs=(tokens, sums, sums, sums),
        check_vma=False,
    )
```

```python
import functools

import jax
import jax.numpy as jnp
from jax import lax
from jax.experimental import pallas as pl
from jax.experimental.pallas import tpu as pltpu
from jax.sharding import PartitionSpec as P

EPS = 1e-6
F32, BF16 = jnp.float32, jnp.bfloat16
MESH = pl.DeviceIdType.MESH
ANY = pl.BlockSpec(memory_space=pl.ANY)
VMEM_LIMIT = 66_000_000


class Place:
    def __init__(self):
        me = lax.axis_index("dp")
        core, z = lax.rem(me, 2), lax.rem(me // 2, 4)
        column = me - 2 * z - core
        y, x = lax.rem(me // 8, 2), me // 16
        self.me, self.core, self.z = me, core, z
        self.partner = me + 1 - 2 * core
        self.by_x, self.by_y = me + 16 - 32 * x, me + 8 - 16 * y
        over_x, over_y = column + 16 - 32 * x, column + 8 - 16 * y
        self.columns = column, over_x, over_y, over_x + 8 - 16 * y
        self.in_z = [column + core + 2 * lax.rem(z + k, 4) for k in range(4)]

    def piece(self, kind, k, core=None):
        core = self.core if core is None else core
        return self.columns[kind] + 2 * lax.rem(self.z + 4 - k, 4) + core

    def greet(self):
        barrier = pltpu.get_barrier_semaphore()
        for other in (self.partner, self.by_x, self.by_y, *self.in_z[1:]):
            pl.semaphore_signal(barrier, inc=1, device_id={"dp": other}, device_id_type=MESH)
        pl.semaphore_wait(barrier, 6)


def remote(src, dst, send, recv, device):
    return pltpu.make_async_remote_copy(
        src_ref=src, dst_ref=dst, send_sem=send, recv_sem=recv, device_id={"dp": device}, device_id_type=MESH
    )


OWN, X, Y, DIAG = range(4)


class Gather:
    def __init__(self, place, src, out, send, recv, pair, local):
        self.place, self.src, self.out = place, src, out
        self.send, self.recv, self.pair, self.local = send, recv, pair, local

    def push(self, src, at, kind, k, device):
        remote(src, self.out.at[at], self.send, self.recv.at[4 * kind + k], device).start()

    def pass_on(self, src, at):
        remote(src, self.out.at[at], self.send, self.pair, self.place.partner).start()

    def start(self):
        place = self.place
        pltpu.make_async_copy(self.src, self.out.at[place.me], self.local).start()
        for k in (1, 2, 3):
            self.push(self.src, place.me, OWN, k, place.in_z[k])
        self.push(self.src, place.me, X, 0, place.by_x)
        self.push(self.src, place.me, Y, 0, place.by_y)
        self.pass_on(self.src, place.me)

    def arrived(self, kind, k):
        at = self.place.piece(kind, k)
        here = self.out.at[at]
        pltpu.make_async_copy(here, here, self.recv.at[4 * kind + k]).wait()
        return here, at

    def along_z(self, k):
        here, at = self.arrived(OWN, k)
        self.push(here, at, X, k, self.place.by_x)
        self.push(here, at, Y, k, self.place.by_y)
        self.pass_on(here, at)

    def across(self, k):
        here, at = self.arrived(X, k)
        if k < 2:
            self.push(here, at, DIAG, k, self.place.by_y)
        self.pass_on(here, at)
        here, at = self.arrived(Y, k)
        if k >= 2:
            self.push(here, at, DIAG, k, self.place.by_x)
        self.pass_on(here, at)

    def diagonal(self, k):
        self.pass_on(*self.arrived(DIAG, k))

    def finish(self):
        pltpu.make_async_copy(self.src, self.src, self.local).wait()
        for n, sem in ((16, self.pair), (31, self.send)):
            some = self.out.at[pl.ds(0, n)]
            pltpu.make_async_copy(some, some, sem).wait()

    def events(self):
        groups = [[functools.partial(self.across, 0)]]
        for k in (1, 2, 3):
            groups += [[functools.partial(self.along_z, k)], [functools.partial(self.across, k)]]
        return groups + [[functools.partial(self.diagonal, k)] for k in range(4)]


GATHER_SEMS = (pltpu.SemaphoreType.DMA, pltpu.SemaphoreType.DMA((16,)), pltpu.SemaphoreType.DMA, pltpu.SemaphoreType.DMA)


def woven(lists, lag):
    order = [(i + lag * n, n, group) for n, groups in enumerate(lists) for i, group in enumerate(groups)]
    return [step for _, _, group in sorted(order, key=lambda t: t[:2]) for step in group]


class Scatter:
    def __init__(self, place, terms, out, columns, mine, got, send, load, pair, cross, local):
        self.place, self.mine, self.got = place, mine, got
        self.terms, self.out = terms.at[:, :, columns], out.at[:, columns]
        self.send, self.load, self.pair, self.cross, self.local = send, load, pair, cross, local

    def start(self):
        place = self.place
        for kind in (DIAG, X, Y, OWN):
            for k in range(4):
                slot = 4 * kind + k
                src = self.terms.at[place.piece(kind, k, 1 - place.core)]
                remote(src, self.got.at[slot], self.send, self.pair.at[kind], place.partner).start()
                pltpu.make_async_copy(self.terms.at[place.piece(kind, k)], self.mine.at[slot], self.load.at[kind]).start()

    def ready(self, kind):
        four = self.mine.at[pl.ds(0, 4)]
        pltpu.make_async_copy(four, four, self.load.at[kind]).wait()
        pltpu.make_async_copy(four, four, self.pair.at[kind]).wait()

    def total(self, kind, k, others):
        slot = 4 * kind + k
        for n in others:
            here = self.got.at[16 + n]
            pltpu.make_async_copy(here, here, self.cross.at[n]).wait()
        total = self.mine[slot].astype(F32) + self.got[slot].astype(F32)
        for n in others:
            total += self.got[16 + n].astype(F32)
        return total.astype(BF16)

    def push(self, kind, k, others, to, device):
        slot = 4 * kind + k
        self.mine[slot] = self.total(kind, k, others)
        remote(self.mine.at[slot], self.got.at[16 + to], self.send, self.cross.at[to], device).start()

    def diagonal(self, k):
        if k == 0:
            self.ready(DIAG)
        self.push(DIAG, k, (), k, self.place.by_x if k < 2 else self.place.by_y)

    def over_x(self, k):
        if k == 0:
            self.ready(X)
        self.push(X, k, () if k < 2 else (k,), 4 + k, self.place.by_x)

    def over_y(self, k):
        if k == 2:
            self.ready(Y)
        self.push(Y, k, (k,) if k < 2 else (), 8 + k, self.place.by_y)

    def along_z(self, k):
        if k == 1:
            self.ready(OWN)
        self.push(OWN, k, (4 + k, 8 + k), 12 + k, self.place.in_z[4 - k])

    def last(self):
        self.mine[0] = self.total(OWN, 0, (4, 8, 13, 14, 15))
        pltpu.make_async_copy(self.mine.at[0], self.out, self.local).start()

    def events(self):
        do = functools.partial
        return [
            [do(self.diagonal, k) for k in (0, 2, 1, 3)],
            [do(self.over_x, 0), do(self.over_y, 2), do(self.over_x, 1), do(self.over_y, 3)],
            [do(self.over_y, 0), do(self.over_x, 2), do(self.over_y, 1), do(self.over_x, 3)],
            [do(self.along_z, k) for k in (1, 2, 3)],
            [self.last],
        ]

    def finish(self):
        pltpu.make_async_copy(self.mine.at[0], self.out, self.local).wait()
        some = self.terms.at[pl.ds(0, 31)]
        pltpu.make_async_copy(some, some, self.send).wait()


PARTS = 2


def cuts(columns):
    at = [128 * (columns // 128 * i // PARTS) for i in range(PARTS + 1)]
    return [(lo, hi - lo) for lo, hi in zip(at, at[1:])]


def scatter_scratch(rows, columns):
    dma = pltpu.SemaphoreType.DMA
    return [
        pltpu.VMEM((16, rows, columns), BF16), pltpu.VMEM((32, rows, columns), BF16), dma, dma((4,)), dma((4,)), dma((16,)), dma
    ]


class Comm:
    def __init__(self, kind, arrays):
        self.kind, self.arrays, self.n = kind, list(arrays), len(arrays)
        if kind == "gather":
            self.shapes = [jax.ShapeDtypeStruct((32, *b.shape), BF16) for b in arrays]
            self.scratch = [s for _ in arrays for s in GATHER_SEMS]
        else:
            self.shapes = [jax.ShapeDtypeStruct(t.shape[1:], BF16) for t in arrays]
            self.scratch = [s for t in arrays for _, width in cuts(t.shape[2]) for s in scatter_scratch(t.shape[1], width)]
        self.specs = [ANY] * self.n

    def make(self, srcs, outs, scratch):
        place = Place()
        if self.kind == "gather":
            return place, [Gather(place, srcs[i], outs[i], *scratch[4 * i : 4 * i + 4]) for i in range(self.n)]
        parts = [(i, pl.ds(lo, width)) for i, t in enumerate(self.arrays) for lo, width in cuts(t.shape[2])]
        return place, [Scatter(place, srcs[i], outs[i], part, *scratch[7 * k : 7 * k + 7]) for k, (i, part) in enumerate(parts)]

    def driver(self, srcs, outs, scratch, step, steps, polls):
        if not self.n:
            return lambda: None, lambda: None
        place, ones = self.make(srcs, outs, scratch)
        events = woven([one.events() for one in ones], 3 if self.kind == "gather" else 1)
        slots, calls = steps * polls, iter(range(polls))

        @pl.when(step == 0)
        def _():
            place.greet()
            for one in ones:
                one.start()

        def poll():
            call = next(calls)
            for i in range(steps):
                slot = i * polls + call
                share = events[len(events) * slot // slots : len(events) * (slot + 1) // slots]
                if share:

                    @pl.when(step == i)
                    def _(share=share):
                        for event in share:
                            event()

        def end():
            @pl.when(step == steps - 1)
            def _():
                for one in ones:
                    one.finish()

        return poll, end


NONE = Comm("gather", ())


def call(body, name, grid, ins, in_specs, outs, out_specs, scratch, comm, number, flops, polls=1):
    n_in, n_out, n_scratch = len(ins), len(outs), len(scratch)

    def kernel(*refs):
        step = pl.program_id(0)
        cut = [n_in, comm.n, n_out, comm.n, n_scratch, len(comm.scratch)]
        groups, at = [], 0
        for c in cut:
            groups.append(refs[at : at + c])
            at += c
        poll, end = comm.driver(groups[1], groups[3], groups[5], step, grid, polls)
        body(step, groups[0], groups[2], groups[4], poll)
        end()

    params = dict(vmem_limit_bytes=VMEM_LIMIT, dimension_semantics=("arbitrary",))
    if comm.n:
        params |= dict(collective_id=number, has_side_effects=True)
    results = pl.pallas_call(
        kernel,
        grid=(grid,),
        out_shape=[*outs, *comm.shapes],
        in_specs=[*in_specs, *comm.specs],
        out_specs=[*out_specs, *comm.specs],
        scratch_shapes=[*scratch, *comm.scratch],
        compiler_params=pltpu.CompilerParams(**params),
        cost_estimate=pl.CostEstimate(flops=flops, bytes_accessed=50_000_000, transcendentals=0),
        name=name,
    )(*ins, *comm.arrays)
    return list(results[:n_out]), list(results[n_out:])


def whole(shape):
    return pl.BlockSpec(shape, lambda i: (0,) * len(shape), pipeline_mode=pl.Buffered(1))


def over(rows, columns):
    return pl.BlockSpec((rows, columns), lambda i: (i, 0))


def across(rows, columns):
    return pl.BlockSpec((rows, columns), lambda i: (0, i))


def like(shape, dtype=BF16):
    return jax.ShapeDtypeStruct(shape, dtype)


def dot(a, b, ca, cb):
    return lax.dot_general(a, b, (((ca,), (cb,)), ((), ())), preferred_element_type=F32)


TILE = 256


def close_up(blocks, out):
    n, rows, _ = blocks.shape

    def pair(i, _):
        two = jnp.concatenate([blocks[2 * i].astype(F32), blocks[2 * i + 1].astype(F32)], 0)
        out[pl.ds(pl.multiple_of(2 * rows * i, 8), 2 * rows), :] = two.astype(BF16)
        return 0

    lax.fori_loop(0, n // 2, pair, 0)


def normed(h):
    wide = h.astype(F32)
    return (wide * lax.rsqrt(jnp.mean(wide**2, -1, keepdims=True) + EPS)).astype(BF16)


def gated(by_p, gate, up):
    s = jax.nn.sigmoid(gate)
    return (by_p * up * (s * (1 + gate * (1 - s)))).astype(BF16), (by_p * (gate * s)).astype(BF16)


def forward(h, wg, wu, comm, number):
    tokens, d = h.shape
    ff = wg.shape[2]
    piece = ff // 3

    def body(step, ins, outs, scratch, poll):
        h_ref, wg_ref, wu_ref = ins
        gate_ref, up_ref, p_ref, pt_ref, at_ref, wg_out, wu_out = outs

        @pl.when(step == 0)
        def _():
            close_up(wg_ref, wg_out)
            close_up(wu_ref, wu_out)

        a = normed(h_ref[...])
        at_ref[...] = a.T
        for c in range(3):
            part = pl.ds(piece * c, piece)
            gate = dot(a, wg_out[:, part], 1, 0)
            up = dot(a, wu_out[:, part], 1, 0)
            gate_ref[:, part] = gate
            up_ref[:, part] = up
            p = (gate * jax.nn.sigmoid(gate) * up).astype(BF16)
            p_ref[:, part] = p
            pt_ref[part, :] = p.T
            if c != 1:
                poll()

    tile_d, tile_ff = over(TILE, d), over(TILE, ff)
    wide, square = like((tokens, ff), F32), like((d, ff))
    return call(
        body, f"forward_{number}", tokens // TILE,
        (h, wg, wu), (tile_d, whole(wg.shape), whole(wu.shape)),
        (wide, wide, like((tokens, ff)), like((ff, tokens)), like((d, tokens)), square, square),
        (tile_ff, tile_ff, tile_ff, across(ff, TILE), across(d, TILE), whole((d, ff)), whole((d, ff))),
        (), comm, number, 4 * tokens * d * ff, polls=2,
    )


def turn(h, p, wd, wg, wu, by_h, wd_last, number):
    tokens, d = h.shape
    ff = wg.shape[2]
    piece = ff // 3

    def body(step, ins, outs, scratch, poll):
        h_ref, p_ref, wd_ref, wg_ref, wu_ref, by_ref, last_ref = ins
        by_gate_ref, by_up_ref, pt_ref, at_ref, wg_out, wu_out, h_out = outs

        @pl.when(step == 0)
        def _():
            close_up(wg_ref, wg_out)
            close_up(wu_ref, wu_out)

        h = h_ref[...] + dot(p_ref[...], wd_ref[...], 1, 0).astype(BF16)
        h_out[...] = h
        a = normed(h)
        at_ref[...] = a.T
        by_h = by_ref[...]
        for c in range(3):
            part = pl.ds(piece * c, piece)
            gate = dot(a, wg_out[:, part], 1, 0)
            up = dot(a, wu_out[:, part], 1, 0)
            by_p = dot(by_h, last_ref[part, :], 1, 1).astype(BF16).astype(F32)
            pt_ref[part, :] = (gate * jax.nn.sigmoid(gate) * up).astype(BF16).T
            by_gate_ref[:, part], by_up_ref[:, part] = gated(by_p, gate, up)

    tile_d, tile_ff, square = over(TILE, d), over(TILE, ff), like((d, ff))
    return call(
        body, f"turn_{number}", tokens // TILE,
        (h, p, wd, wg, wu, by_h, wd_last),
        (tile_d, tile_ff, whole(wd.shape), whole(wg.shape), whole(wu.shape), tile_d, whole(wd.shape)),
        (like((tokens, ff)), like((tokens, ff)), like((ff, tokens)), like((d, tokens)), square, square, like(h.shape)),
        (tile_ff, tile_ff, across(ff, TILE), across(d, TILE), whole((d, ff)), whole((d, ff)), tile_d),
        (), NONE, number, 8 * tokens * d * ff,
    )[0]


def backward(by_h, later, earlier, comm, number):
    tokens, d = by_h.shape
    tile_d = over(TILE, d)
    ff = (later[1] if later else earlier[0]).shape[1]
    tile_ff = over(TILE, ff)
    piece = ff // 3

    def body(step, ins, outs, scratch, poll):
        by_ref, *ins = ins
        outs = list(outs)
        by_h = by_ref[...]
        poll()
        if later:
            h_ref, by_gate_ref, by_up_ref, wg_ref, wu_ref = ins[:5]
            by_a = dot(by_gate_ref[...], wg_ref[...], 1, 1).astype(BF16)
            by_a = (by_a + dot(by_up_ref[...], wu_ref[...], 1, 1).astype(BF16)).astype(F32)
            poll()
            wide = h_ref[...].astype(F32)
            scale = lax.rsqrt(jnp.mean(wide**2, -1, keepdims=True) + EPS)
            inner = jnp.mean(by_a * wide, -1, keepdims=True)
            by_h = by_h + (scale * (by_a - wide * (scale * scale * inner))).astype(BF16)
            outs.pop(0)[...] = by_h
        if earlier:
            gate_ref, up_ref, wd_ref = ins[-3:]
            for c in range(3):
                part = pl.ds(piece * c, piece)
                by_p = dot(by_h, wd_ref[part, :], 1, 1).astype(BF16).astype(F32)
                by_gate, by_up = gated(by_p, gate_ref[:, part], up_ref[:, part])
                outs[0][:, part] = by_gate
                outs[1][:, part] = by_up
            poll()

    ins, in_specs, outs, out_specs, polls = [by_h], [tile_d], [], [], 1
    if later:
        ins += later
        in_specs += [tile_d, tile_ff, tile_ff, whole((d, ff)), whole((d, ff))]
        outs.append(like((tokens, d)))
        out_specs.append(tile_d)
        polls += 1
    if earlier:
        ins += earlier
        in_specs += [tile_ff, tile_ff, whole((ff, d))]
        outs += [like((tokens, ff))] * 2
        out_specs += [tile_ff] * 2
        polls += 1
    flops = (4 * bool(later) + 2 * bool(earlier)) * tokens * d * ff
    return call(body, f"backward_{number}", tokens // TILE, ins, in_specs, outs, out_specs, (), comm, number, flops, polls)


def weight_terms(at, pt, by_gate, by_up, by_h, rows, number):
    d, tokens = at.shape
    ff = pt.shape[0]
    n = d // rows

    def body(step, ins, outs, scratch, poll):
        at_ref, pt_ref, by_gate_ref, by_up_ref, by_h_ref = ins
        wg_ref, wu_ref, wd_ref = outs
        for by_ref, w_ref in ((by_gate_ref, wg_ref), (by_up_ref, wu_ref)):
            term = dot(at_ref[...], by_ref[...], 1, 0)
            for j in range(n):
                w_ref[j] = term[rows * j : rows * j + rows].astype(BF16)
        wd_ref[...] = dot(pt_ref[...], by_h_ref[...], 1, 0).astype(BF16)

    blocks = pl.BlockSpec((n, rows, TILE), lambda i: (0, 0, i))
    wg, wu, wd = call(
        body, f"weight_terms_{number}", ff // TILE,
        (at, pt, by_gate, by_up, by_h),
        (whole(at.shape), over(TILE, tokens), across(tokens, TILE), across(tokens, TILE), whole(by_h.shape)),
        (like((n, rows, ff)), like((n, rows, ff)), like((ff, d))),
        (blocks, blocks, over(TILE, d)),
        (), NONE, number, 6 * tokens * d * ff,
    )[0]
    return wg, wu, wd.reshape(n, ff // n, d)


def gather_first(blocks):
    def body(step, ins, outs, scratch, poll):
        poll()

    return call(body, "gather_first", 1, (), (), (), (), (), Comm("gather", blocks), 0, 0)[1]


def solution(mesh):
    def step(x, dy, w_gate, w_up, w_down):
        rows, ff = w_gate.shape[1:]
        d = w_down.shape[2]

        x, dy = x[0], dy[0]
        wg0, wu0 = gather_first((w_gate[0], w_up[0]))
        (gate0, up0, p0, pt0, at0, wg0, wu0), (wd0, wg1, wu1, wd1) = forward(
            x, wg0, wu0, Comm("gather", (w_down[0], w_gate[1], w_up[1], w_down[1])), 1
        )
        wd0, wd1 = wd0.reshape(ff, d), wd1.reshape(ff, d)
        by_gate1, by_up1, pt1, at1, wg1, wu1, h1 = turn(x, p0, wd0, wg1, wu1, dy, wd1, 2)
        terms = weight_terms(at1, pt1, by_gate1, by_up1, dy, rows, 3)
        (by_h, by_gate0, by_up0), (sum_g1, sum_u1, sum_d1) = backward(
            dy, (h1, by_gate1, by_up1, wg1, wu1), (gate0, up0, wd0), Comm("scatter", terms), 4
        )
        terms = weight_terms(at0, pt0, by_gate0, by_up0, by_h, rows, 5)
        (by_x,), (sum_g0, sum_u0, sum_d0) = backward(by_h, (x, by_gate0, by_up0, wg0, wu0), (), Comm("scatter", terms), 6)
        return by_x[None], jnp.stack([sum_g0, sum_g1]), jnp.stack([sum_u0, sum_u1]), jnp.stack([sum_d0, sum_d1])

    tokens, weights = P(("rep", "dp"), None, None), P(None, "dp", None)
    sums = P("rep", "dp", None)
    return jax.shard_map(
        step,
        mesh=mesh,
        in_specs=(tokens, tokens, weights, weights, weights),
        out_specs=(tokens, sums, sums, sums),
        check_vma=False,
    )
```

```python
import functools

import jax
import jax.numpy as jnp
from jax import lax
from jax.experimental import pallas as pl
from jax.experimental.pallas import tpu as pltpu
from jax.sharding import PartitionSpec as P

EPS = 1e-6
F32, BF16 = jnp.float32, jnp.bfloat16
MESH = pl.DeviceIdType.MESH
ANY = pl.BlockSpec(memory_space=pl.ANY)
VMEM_LIMIT = 66_000_000


class Place:
    def __init__(self):
        me = lax.axis_index("dp")
        core, z = lax.rem(me, 2), lax.rem(me // 2, 4)
        column = me - 2 * z - core
        y, x = lax.rem(me // 8, 2), me // 16
        self.me, self.core, self.z = me, core, z
        self.partner = me + 1 - 2 * core
        self.by_x, self.by_y = me + 16 - 32 * x, me + 8 - 16 * y
        over_x, over_y = column + 16 - 32 * x, column + 8 - 16 * y
        self.columns = column, over_x, over_y, over_x + 8 - 16 * y
        self.in_z = [column + core + 2 * lax.rem(z + k, 4) for k in range(4)]

    def piece(self, kind, k, core=None):
        core = self.core if core is None else core
        return self.columns[kind] + 2 * lax.rem(self.z + 4 - k, 4) + core

    def greet(self):
        barrier = pltpu.get_barrier_semaphore()
        for other in (self.partner, self.by_x, self.by_y, *self.in_z[1:]):
            pl.semaphore_signal(barrier, inc=1, device_id={"dp": other}, device_id_type=MESH)
        pl.semaphore_wait(barrier, 6)


def remote(src, dst, send, recv, device):
    return pltpu.make_async_remote_copy(
        src_ref=src, dst_ref=dst, send_sem=send, recv_sem=recv, device_id={"dp": device}, device_id_type=MESH
    )


OWN, X, Y, DIAG = range(4)


class Gather:
    def __init__(self, place, src, out, send, recv, pair, local):
        self.place, self.src, self.out = place, src, out
        self.send, self.recv, self.pair, self.local = send, recv, pair, local

    def push(self, src, at, kind, k, device):
        remote(src, self.out.at[at], self.send, self.recv.at[4 * kind + k], device).start()

    def pass_on(self, src, at):
        remote(src, self.out.at[at], self.send, self.pair, self.place.partner).start()

    def start(self):
        place = self.place
        pltpu.make_async_copy(self.src, self.out.at[place.me], self.local).start()
        for k in (1, 2, 3):
            self.push(self.src, place.me, OWN, k, place.in_z[k])
        self.push(self.src, place.me, X, 0, place.by_x)
        self.push(self.src, place.me, Y, 0, place.by_y)
        self.pass_on(self.src, place.me)

    def arrived(self, kind, k):
        at = self.place.piece(kind, k)
        here = self.out.at[at]
        pltpu.make_async_copy(here, here, self.recv.at[4 * kind + k]).wait()
        return here, at

    def along_z(self, k):
        here, at = self.arrived(OWN, k)
        self.push(here, at, X, k, self.place.by_x)
        self.push(here, at, Y, k, self.place.by_y)
        self.pass_on(here, at)

    def across(self, k):
        here, at = self.arrived(X, k)
        if k < 2:
            self.push(here, at, DIAG, k, self.place.by_y)
        self.pass_on(here, at)
        here, at = self.arrived(Y, k)
        if k >= 2:
            self.push(here, at, DIAG, k, self.place.by_x)
        self.pass_on(here, at)

    def diagonal(self, k):
        self.pass_on(*self.arrived(DIAG, k))

    def finish(self):
        pltpu.make_async_copy(self.src, self.src, self.local).wait()
        for n, sem in ((16, self.pair), (31, self.send)):
            some = self.out.at[pl.ds(0, n)]
            pltpu.make_async_copy(some, some, sem).wait()

    def events(self):
        groups = [[functools.partial(self.across, 0)]]
        for k in (1, 2, 3):
            groups += [[functools.partial(self.along_z, k)], [functools.partial(self.across, k)]]
        return groups + [[functools.partial(self.diagonal, k)] for k in range(4)]


GATHER_SEMS = (pltpu.SemaphoreType.DMA, pltpu.SemaphoreType.DMA((16,)), pltpu.SemaphoreType.DMA, pltpu.SemaphoreType.DMA)


def woven(lists, lag):
    order = [(i + lag * n, n, group) for n, groups in enumerate(lists) for i, group in enumerate(groups)]
    return [step for _, _, group in sorted(order, key=lambda t: t[:2]) for step in group]


class Scatter:
    def __init__(self, place, terms, out, columns, mine, got, send, load, pair, cross, local):
        self.place, self.mine, self.got = place, mine, got
        self.terms, self.out = terms.at[:, :, columns], out.at[:, columns]
        self.send, self.load, self.pair, self.cross, self.local = send, load, pair, cross, local

    def start(self):
        place = self.place
        for kind in (DIAG, X, Y, OWN):
            for k in range(4):
                slot = 4 * kind + k
                src = self.terms.at[place.piece(kind, k, 1 - place.core)]
                remote(src, self.got.at[slot], self.send, self.pair.at[kind], place.partner).start()
                pltpu.make_async_copy(self.terms.at[place.piece(kind, k)], self.mine.at[slot], self.load.at[kind]).start()

    def ready(self, kind):
        four = self.mine.at[pl.ds(0, 4)]
        pltpu.make_async_copy(four, four, self.load.at[kind]).wait()
        pltpu.make_async_copy(four, four, self.pair.at[kind]).wait()

    def total(self, kind, k, others):
        slot = 4 * kind + k
        for n in others:
            here = self.got.at[16 + n]
            pltpu.make_async_copy(here, here, self.cross.at[n]).wait()
        total = self.mine[slot].astype(F32) + self.got[slot].astype(F32)
        for n in others:
            total += self.got[16 + n].astype(F32)
        return total.astype(BF16)

    def push(self, kind, k, others, to, device):
        slot = 4 * kind + k
        self.mine[slot] = self.total(kind, k, others)
        remote(self.mine.at[slot], self.got.at[16 + to], self.send, self.cross.at[to], device).start()

    def diagonal(self, k):
        if k == 0:
            self.ready(DIAG)
        self.push(DIAG, k, (), k, self.place.by_x if k < 2 else self.place.by_y)

    def over_x(self, k):
        if k == 0:
            self.ready(X)
        self.push(X, k, () if k < 2 else (k,), 4 + k, self.place.by_x)

    def over_y(self, k):
        if k == 2:
            self.ready(Y)
        self.push(Y, k, (k,) if k < 2 else (), 8 + k, self.place.by_y)

    def along_z(self, k):
        if k == 1:
            self.ready(OWN)
        self.push(OWN, k, (4 + k, 8 + k), 12 + k, self.place.in_z[4 - k])

    def last(self):
        self.mine[0] = self.total(OWN, 0, (4, 8, 13, 14, 15))
        pltpu.make_async_copy(self.mine.at[0], self.out, self.local).start()

    def events(self):
        do = functools.partial
        return [
            [do(self.diagonal, k) for k in (0, 2, 1, 3)],
            [do(self.over_x, 0), do(self.over_y, 2), do(self.over_x, 1), do(self.over_y, 3)],
            [do(self.over_y, 0), do(self.over_x, 2), do(self.over_y, 1), do(self.over_x, 3)],
            [do(self.along_z, k) for k in (1, 2, 3)],
            [self.last],
        ]

    def finish(self):
        pltpu.make_async_copy(self.mine.at[0], self.out, self.local).wait()
        some = self.terms.at[pl.ds(0, 31)]
        pltpu.make_async_copy(some, some, self.send).wait()


PARTS = 3


def cuts(columns):
    at = [128 * (columns // 128 * i // PARTS) for i in range(PARTS + 1)]
    return [(lo, hi - lo) for lo, hi in zip(at, at[1:])]


def scatter_scratch(rows, columns):
    dma = pltpu.SemaphoreType.DMA
    return [
        pltpu.VMEM((16, rows, columns), BF16), pltpu.VMEM((32, rows, columns), BF16), dma, dma((4,)), dma((4,)), dma((16,)), dma
    ]


class Comm:
    def __init__(self, kind, arrays):
        self.kind, self.arrays, self.n = kind, list(arrays), len(arrays)
        if kind == "gather":
            self.shapes = [jax.ShapeDtypeStruct((32, *b.shape), BF16) for b in arrays]
            self.scratch = [s for _ in arrays for s in GATHER_SEMS]
        else:
            self.shapes = [jax.ShapeDtypeStruct(t.shape[1:], BF16) for t in arrays]
            self.scratch = [s for t in arrays for _, width in cuts(t.shape[2]) for s in scatter_scratch(t.shape[1], width)]
        self.specs = [ANY] * self.n

    def make(self, srcs, outs, scratch):
        place = Place()
        if self.kind == "gather":
            return place, [Gather(place, srcs[i], outs[i], *scratch[4 * i : 4 * i + 4]) for i in range(self.n)]
        parts = [(i, pl.ds(lo, width)) for i, t in enumerate(self.arrays) for lo, width in cuts(t.shape[2])]
        return place, [Scatter(place, srcs[i], outs[i], part, *scratch[7 * k : 7 * k + 7]) for k, (i, part) in enumerate(parts)]

    def driver(self, srcs, outs, scratch, step, steps, polls):
        if not self.n:
            return lambda: None, lambda: None
        place, ones = self.make(srcs, outs, scratch)
        events = woven([one.events() for one in ones], 3 if self.kind == "gather" else 1)
        slots, calls = steps * polls, iter(range(polls))

        @pl.when(step == 0)
        def _():
            place.greet()
            for one in ones:
                one.start()

        def poll():
            call = next(calls)
            for i in range(steps):
                slot = i * polls + call
                share = events[len(events) * slot // slots : len(events) * (slot + 1) // slots]
                if share:

                    @pl.when(step == i)
                    def _(share=share):
                        for event in share:
                            event()

        def end():
            @pl.when(step == steps - 1)
            def _():
                for one in ones:
                    one.finish()

        return poll, end


NONE = Comm("gather", ())


def call(body, name, grid, ins, in_specs, outs, out_specs, scratch, comm, number, flops, polls=1):
    n_in, n_out, n_scratch = len(ins), len(outs), len(scratch)

    def kernel(*refs):
        step = pl.program_id(0)
        cut = [n_in, comm.n, n_out, comm.n, n_scratch, len(comm.scratch)]
        groups, at = [], 0
        for c in cut:
            groups.append(refs[at : at + c])
            at += c
        poll, end = comm.driver(groups[1], groups[3], groups[5], step, grid, polls)
        body(step, groups[0], groups[2], groups[4], poll)
        end()

    params = dict(vmem_limit_bytes=VMEM_LIMIT, dimension_semantics=("arbitrary",))
    if comm.n:
        params |= dict(collective_id=number, has_side_effects=True)
    results = pl.pallas_call(
        kernel,
        grid=(grid,),
        out_shape=[*outs, *comm.shapes],
        in_specs=[*in_specs, *comm.specs],
        out_specs=[*out_specs, *comm.specs],
        scratch_shapes=[*scratch, *comm.scratch],
        compiler_params=pltpu.CompilerParams(**params),
        cost_estimate=pl.CostEstimate(flops=flops, bytes_accessed=50_000_000, transcendentals=0),
        name=name,
    )(*ins, *comm.arrays)
    return list(results[:n_out]), list(results[n_out:])


def whole(shape):
    return pl.BlockSpec(shape, lambda i: (0,) * len(shape), pipeline_mode=pl.Buffered(1))


def over(rows, columns):
    return pl.BlockSpec((rows, columns), lambda i: (i, 0))


def across(rows, columns):
    return pl.BlockSpec((rows, columns), lambda i: (0, i))


def like(shape, dtype=BF16):
    return jax.ShapeDtypeStruct(shape, dtype)


def dot(a, b, ca, cb):
    return lax.dot_general(a, b, (((ca,), (cb,)), ((), ())), preferred_element_type=F32)


TILE = 256


def close_up(blocks, out):
    n, rows, _ = blocks.shape

    def pair(i, _):
        two = jnp.concatenate([blocks[2 * i].astype(F32), blocks[2 * i + 1].astype(F32)], 0)
        out[pl.ds(pl.multiple_of(2 * rows * i, 8), 2 * rows), :] = two.astype(BF16)
        return 0

    lax.fori_loop(0, n // 2, pair, 0)


def normed(h):
    wide = h.astype(F32)
    return (wide * lax.rsqrt(jnp.mean(wide**2, -1, keepdims=True) + EPS)).astype(BF16)


def gated(by_p, gate, up):
    s = jax.nn.sigmoid(gate)
    return (by_p * up * (s * (1 + gate * (1 - s)))).astype(BF16), (by_p * (gate * s)).astype(BF16)


def forward(h, wg, wu, comm, number):
    tokens, d = h.shape
    ff = wg.shape[2]
    piece = ff // 3

    def body(step, ins, outs, scratch, poll):
        h_ref, wg_ref, wu_ref = ins
        gate_ref, up_ref, p_ref, pt_ref, at_ref, wg_out, wu_out = outs

        @pl.when(step == 0)
        def _():
            close_up(wg_ref, wg_out)
            close_up(wu_ref, wu_out)

        a = normed(h_ref[...])
        at_ref[...] = a.T
        for c in range(3):
            part = pl.ds(piece * c, piece)
            gate = dot(a, wg_out[:, part], 1, 0)
            up = dot(a, wu_out[:, part], 1, 0)
            gate_ref[:, part] = gate
            up_ref[:, part] = up
            p = (gate * jax.nn.sigmoid(gate) * up).astype(BF16)
            p_ref[:, part] = p
            pt_ref[part, :] = p.T
            if c != 1:
                poll()

    tile_d, tile_ff = over(TILE, d), over(TILE, ff)
    wide, square = like((tokens, ff), F32), like((d, ff))
    return call(
        body, f"forward_{number}", tokens // TILE,
        (h, wg, wu), (tile_d, whole(wg.shape), whole(wu.shape)),
        (wide, wide, like((tokens, ff)), like((ff, tokens)), like((d, tokens)), square, square),
        (tile_ff, tile_ff, tile_ff, across(ff, TILE), across(d, TILE), whole((d, ff)), whole((d, ff))),
        (), comm, number, 4 * tokens * d * ff, polls=2,
    )


def turn(h, p, wd, wg, wu, by_h, wd_last, number):
    tokens, d = h.shape
    ff = wg.shape[2]
    piece = ff // 3

    def body(step, ins, outs, scratch, poll):
        h_ref, p_ref, wd_ref, wg_ref, wu_ref, by_ref, last_ref = ins
        by_gate_ref, by_up_ref, pt_ref, at_ref, wg_out, wu_out, h_out = outs

        @pl.when(step == 0)
        def _():
            close_up(wg_ref, wg_out)
            close_up(wu_ref, wu_out)

        h = h_ref[...] + dot(p_ref[...], wd_ref[...], 1, 0).astype(BF16)
        h_out[...] = h
        a = normed(h)
        at_ref[...] = a.T
        by_h = by_ref[...]
        for c in range(3):
            part = pl.ds(piece * c, piece)
            gate = dot(a, wg_out[:, part], 1, 0)
            up = dot(a, wu_out[:, part], 1, 0)
            by_p = dot(by_h, last_ref[part, :], 1, 1).astype(BF16).astype(F32)
            pt_ref[part, :] = (gate * jax.nn.sigmoid(gate) * up).astype(BF16).T
            by_gate_ref[:, part], by_up_ref[:, part] = gated(by_p, gate, up)

    tile_d, tile_ff, square = over(TILE, d), over(TILE, ff), like((d, ff))
    return call(
        body, f"turn_{number}", tokens // TILE,
        (h, p, wd, wg, wu, by_h, wd_last),
        (tile_d, tile_ff, whole(wd.shape), whole(wg.shape), whole(wu.shape), tile_d, whole(wd.shape)),
        (like((tokens, ff)), like((tokens, ff)), like((ff, tokens)), like((d, tokens)), square, square, like(h.shape)),
        (tile_ff, tile_ff, across(ff, TILE), across(d, TILE), whole((d, ff)), whole((d, ff)), tile_d),
        (), NONE, number, 8 * tokens * d * ff,
    )[0]


def backward(by_h, later, earlier, comm, number):
    tokens, d = by_h.shape
    tile_d = over(TILE, d)
    ff = (later[1] if later else earlier[0]).shape[1]
    tile_ff = over(TILE, ff)
    piece = ff // 3

    def body(step, ins, outs, scratch, poll):
        by_ref, *ins = ins
        outs = list(outs)
        by_h = by_ref[...]
        poll()
        if later:
            h_ref, by_gate_ref, by_up_ref, wg_ref, wu_ref = ins[:5]
            by_a = dot(by_gate_ref[...], wg_ref[...], 1, 1).astype(BF16)
            by_a = (by_a + dot(by_up_ref[...], wu_ref[...], 1, 1).astype(BF16)).astype(F32)
            poll()
            wide = h_ref[...].astype(F32)
            scale = lax.rsqrt(jnp.mean(wide**2, -1, keepdims=True) + EPS)
            inner = jnp.mean(by_a * wide, -1, keepdims=True)
            by_h = by_h + (scale * (by_a - wide * (scale * scale * inner))).astype(BF16)
            outs.pop(0)[...] = by_h
        if earlier:
            gate_ref, up_ref, wd_ref = ins[-3:]
            for c in range(3):
                part = pl.ds(piece * c, piece)
                by_p = dot(by_h, wd_ref[part, :], 1, 1).astype(BF16).astype(F32)
                by_gate, by_up = gated(by_p, gate_ref[:, part], up_ref[:, part])
                outs[0][:, part] = by_gate
                outs[1][:, part] = by_up
            poll()

    ins, in_specs, outs, out_specs, polls = [by_h], [tile_d], [], [], 1
    if later:
        ins += later
        in_specs += [tile_d, tile_ff, tile_ff, whole((d, ff)), whole((d, ff))]
        outs.append(like((tokens, d)))
        out_specs.append(tile_d)
        polls += 1
    if earlier:
        ins += earlier
        in_specs += [tile_ff, tile_ff, whole((ff, d))]
        outs += [like((tokens, ff))] * 2
        out_specs += [tile_ff] * 2
        polls += 1
    flops = (4 * bool(later) + 2 * bool(earlier)) * tokens * d * ff
    return call(body, f"backward_{number}", tokens // TILE, ins, in_specs, outs, out_specs, (), comm, number, flops, polls)


def weight_terms(at, pt, by_gate, by_up, by_h, rows, number):
    d, tokens = at.shape
    ff = pt.shape[0]
    n = d // rows

    def body(step, ins, outs, scratch, poll):
        at_ref, pt_ref, by_gate_ref, by_up_ref, by_h_ref = ins
        wg_ref, wu_ref, wd_ref = outs
        for by_ref, w_ref in ((by_gate_ref, wg_ref), (by_up_ref, wu_ref)):
            term = dot(at_ref[...], by_ref[...], 1, 0)
            for j in range(n):
                w_ref[j] = term[rows * j : rows * j + rows].astype(BF16)
        wd_ref[...] = dot(pt_ref[...], by_h_ref[...], 1, 0).astype(BF16)

    blocks = pl.BlockSpec((n, rows, TILE), lambda i: (0, 0, i))
    wg, wu, wd = call(
        body, f"weight_terms_{number}", ff // TILE,
        (at, pt, by_gate, by_up, by_h),
        (whole(at.shape), over(TILE, tokens), across(tokens, TILE), across(tokens, TILE), whole(by_h.shape)),
        (like((n, rows, ff)), like((n, rows, ff)), like((ff, d))),
        (blocks, blocks, over(TILE, d)),
        (), NONE, number, 6 * tokens * d * ff,
    )[0]
    return wg, wu, wd.reshape(n, ff // n, d)


def gather_first(blocks):
    def body(step, ins, outs, scratch, poll):
        poll()

    return call(body, "gather_first", 1, (), (), (), (), (), Comm("gather", blocks), 0, 0)[1]


def solution(mesh):
    def step(x, dy, w_gate, w_up, w_down):
        rows, ff = w_gate.shape[1:]
        d = w_down.shape[2]

        x, dy = x[0], dy[0]
        wg0, wu0 = gather_first((w_gate[0], w_up[0]))
        (gate0, up0, p0, pt0, at0, wg0, wu0), (wd0, wg1, wu1, wd1) = forward(
            x, wg0, wu0, Comm("gather", (w_down[0], w_gate[1], w_up[1], w_down[1])), 1
        )
        wd0, wd1 = wd0.reshape(ff, d), wd1.reshape(ff, d)
        by_gate1, by_up1, pt1, at1, wg1, wu1, h1 = turn(x, p0, wd0, wg1, wu1, dy, wd1, 2)
        terms = weight_terms(at1, pt1, by_gate1, by_up1, dy, rows, 3)
        (by_h, by_gate0, by_up0), (sum_g1, sum_u1, sum_d1) = backward(
            dy, (h1, by_gate1, by_up1, wg1, wu1), (gate0, up0, wd0), Comm("scatter", terms), 4
        )
        terms = weight_terms(at0, pt0, by_gate0, by_up0, by_h, rows, 5)
        (by_x,), (sum_g0, sum_u0, sum_d0) = backward(by_h, (x, by_gate0, by_up0, wg0, wu0), (), Comm("scatter", terms), 6)
        return by_x[None], jnp.stack([sum_g0, sum_g1]), jnp.stack([sum_u0, sum_u1]), jnp.stack([sum_d0, sum_d1])

    tokens, weights = P(("rep", "dp"), None, None), P(None, "dp", None)
    sums = P("rep", "dp", None)
    return jax.shard_map(
        step,
        mesh=mesh,
        in_specs=(tokens, tokens, weights, weights, weights),
        out_specs=(tokens, sums, sums, sums),
        check_vma=False,
    )
```
